32 devices in a mesh: row: 8 (over y, x, core), col: 4 (over z).
Axes of the slice: x: 2, y: 2, z: 4, core: 2. Of those that a mesh axis runs over, the one named last changes fastest.
Arguments:
- temps: bfloat16 [12, 64, 16384], P(None, None, ('row', 'col')), may hold values from -6 to 6
- sensors: int32 [12, 512], replicated, may hold values from 0 to 16383
Outputs:
- corr: bfloat16 [512, 16384], P('col', 'row')
The draws below stay inside these ranges and needn't reach their ends.
Inputs may be any that keep to these rules, and one draw needn't show every extreme that they name: `sensors`: each entry is a pixel index of its tier; candidates may repeat.
All inputs are finite; a program needn't handle non-finite values.
Results may differ from the reference program's by a relative error of at most 0.001.
Values may be sent and summed in bfloat16 or wider, within the bound.
A program may use at most 64 MiB of HBM per device.

```python
import jax
import jax.numpy as jnp
from jax import lax

TIERS = 12
SNAP = 64
PIX_DEV = 512
PIX = 16384
SENS = 512
N_ROW = 8
N_COL = 4


def with_ends(values, stream_key, low, top_value):
    longest = values.shape.index(max(values.shape))
    spots = []
    for shift in (0, 1):
        where = [jax.random.randint(jax.random.fold_in(stream_key, axis), (), 0, length) for axis, length in enumerate(values.shape)]
        where[longest] = (where[longest] + shift) % values.shape[longest]
        spots.append(tuple(where))
    return values.at[spots[0]].set(low).at[spots[1]].set(top_value)


def block_levels(own_key, dims, cuts, low, largest):
    def one(axis_at, parts):
        heights = jax.random.uniform(jax.random.fold_in(jax.random.fold_in(own_key, 6), axis_at), (parts,), jnp.float32, low / len(cuts), largest / len(cuts))
        return jnp.repeat(jnp.exp(heights), dims[axis_at] // parts).reshape((-1,) + (1,) * (len(dims) - axis_at - 1))

    loudness = one(*cuts[0])
    for cut in cuts[1:]:
        loudness = loudness * one(*cut)
    return loudness


def centred(own_key, shape, spread, reach, cuts=(), kind=jnp.bfloat16):
    array = jax.random.normal(own_key, shape, jnp.float32) * spread
    if len(cuts) > 0:
        array = block_levels(own_key, shape, cuts, -0.22, 0.18) * array
    return jnp.clip(array, min=-reach, max=reach).astype(kind)


def setup_inputs(seed: int = 0) -> dict:
    keys = jax.random.split(jax.random.key(seed), 3)
    return {
        "temps": centred(keys[0], (TIERS, SNAP, PIX), 1.0, 6.0, ((2, 32),)),
        "sensors": with_ends(jax.random.randint(keys[1], (TIERS, SENS), 0, PIX), jax.random.fold_in(keys[1], 1), 0, PIX - 1).astype(jnp.int32),
    }


def reference(temps, sensors):
    readings = jax.vmap(lambda fields, cols: jnp.take(fields, cols, axis=1))(temps, sensors)
    chosen = readings.astype(jnp.float32)
    block_width = PIX_DEV * N_COL
    scale_factor = 1.0 / jnp.sqrt(jnp.float32(TIERS * SNAP))

    def one_block(block_index):
        first_pixel = (block_index * block_width).astype(jnp.int32)
        fields = lax.dynamic_slice_in_dim(temps, first_pixel, block_width, 2).astype(jnp.float32)
        summed = jnp.einsum('tsc,tsp->cp', chosen, fields)
        return (summed * scale_factor).astype(jnp.bfloat16)
    blocks = lax.map(one_block, jnp.arange(N_ROW, dtype=jnp.int32))
    return jnp.transpose(blocks, (1, 0, 2)).reshape(SENS, PIX)
```

```python
import functools

import jax
import numpy as np
import jax.numpy as jnp
from jax import lax
from jax.experimental import pallas as pl
from jax.experimental.pallas import tpu as pltpu
from jax.sharding import PartitionSpec as P

SUB = 16
MESH = pl.DeviceIdType.MESH


def kernel(
    n_row, n_col, n_chunk, tiers,
    temps_ref, sens_ref, out_ref,
    sens_t, part, rs_buf, z_src, z_buf, full, out_buf,
    rs_send, rs_recv, z_send, z_recv, ag_send, ag_recv, o_send, o_recv,
):
    r = lax.axis_index("row")
    z = lax.axis_index("col")
    snaps, width = temps_ref.shape[0] // tiers, temps_ref.shape[1]
    depth = temps_ref.shape[0]
    rows_col = out_ref.shape[0] // n_chunk
    rows_chunk = n_row * SUB
    scale = float(np.float32(1.0) / np.sqrt(np.float32(depth)))

    def row_peer(d):
        return lax.rem(r + d, n_row)

    def col_peer(e):
        return lax.rem(z + e, n_col)

    barrier = pltpu.get_barrier_semaphore()
    for d in range(1, n_row):
        pl.semaphore_signal(barrier, inc=1, device_id=(row_peer(d), z), device_id_type=MESH)
    for e in range(1, n_col):
        pl.semaphore_signal(barrier, inc=1, device_id=(r, col_peer(e)), device_id_type=MESH)

    first_pixel = (r * n_col + z) * width
    offsets = jnp.transpose(sens_ref[...] - first_pixel)
    sens_t[...] = offsets.reshape(sens_t.shape)
    pixel_ids = lax.broadcasted_iota(jnp.int32, (rows_chunk, width), 1)

    def select(k):
        mine = sens_t[:, k].reshape(rows_chunk, tiers)
        for t in range(0, tiers, 2):
            pair = []
            for u in (t, t + 1):
                hot = (pixel_ids == mine[:, u:u + 1]).astype(jnp.float32).astype(jnp.bfloat16)
                pair.append(lax.dot_general(
                    hot, temps_ref[u * snaps:(u + 1) * snaps, :],
                    (((1,), (1,)), ((), ())), preferred_element_type=jnp.float32,
                ))
            both = jnp.concatenate(pair, axis=1).astype(jnp.bfloat16)
            part[k, :, :, t * snaps:(t + 2) * snaps] = both.reshape(n_row, SUB, 2 * snaps)

    def start_rs(k):
        for d in range(1, n_row):
            peer = row_peer(d)
            pltpu.make_async_remote_copy(
                part.at[k, peer], rs_buf.at[k, d - 1], rs_send.at[k], rs_recv.at[k],
                device_id=(peer, z), device_id_type=MESH,
            ).start()

    def wait_all(ref, sem):
        pltpu.make_async_copy(ref, ref, sem).wait()

    def start_z(k):
        wait_all(rs_buf.at[k], rs_recv.at[k])
        total = part[k, r]
        for d in range(n_row - 1):
            total = total + rs_buf[k, d]
        z_src[k] = total
        for e in range(1, n_col):
            pltpu.make_async_remote_copy(
                z_src.at[k], z_buf.at[k, e - 1], z_send.at[k], z_recv.at[k],
                device_id=(r, col_peer(e)), device_id_type=MESH,
            ).start()

    def start_ag(k):
        wait_all(z_buf.at[k], z_recv.at[k])
        total = z_src[k]
        for e in range(n_col - 1):
            total = total + z_buf[k, e]
        full[k, r] = total
        for d in range(1, n_row):
            pltpu.make_async_remote_copy(
                full.at[k, r], full.at[k, r], ag_send.at[k], ag_recv.at[k],
                device_id=(row_peer(d), z), device_id_type=MESH,
            ).start()

    def start_out(k):
        wait_all(full.at[k, pl.ds(0, n_row - 1)], ag_recv.at[k])
        readings = full[k].reshape(rows_chunk, depth)
        summed = jnp.dot(readings, temps_ref[...], preferred_element_type=jnp.float32)
        out_buf[k] = (summed * scale).astype(jnp.bfloat16).reshape(n_col, rows_col, width)
        columns = pl.ds(pl.multiple_of(z * width, width), width)
        for e in range(1, n_col):
            peer = col_peer(e)
            pltpu.make_async_remote_copy(
                out_buf.at[k, peer], out_ref.at[pl.ds(k * rows_col, rows_col), columns],
                o_send.at[k], o_recv.at[k],
                device_id=(r, peer), device_id_type=MESH,
            ).start()
        out_ref[pl.ds(k * rows_col, rows_col), columns] = out_buf[k, z]

    select(0)
    pl.semaphore_wait(barrier, n_row + n_col - 2)
    start_rs(0)
    for k in range(1, n_chunk):
        select(k)
        start_rs(k)
    for step in range(n_chunk + 2):
        if step < n_chunk:
            start_z(step)
        if 0 <= step - 1 < n_chunk:
            start_ag(step - 1)
        if 0 <= step - 2 < n_chunk:
            start_out(step - 2)
    for k in range(n_chunk):
        wait_all(out_buf.at[k, pl.ds(0, n_col - 1)], o_recv.at[k])
        wait_all(rs_buf.at[k], rs_send.at[k])
        wait_all(z_buf.at[k], z_send.at[k])
        wait_all(full.at[k, pl.ds(0, n_row - 1)], ag_send.at[k])
        wait_all(out_buf.at[k, pl.ds(0, n_col - 1)], o_send.at[k])


def body(n_row, n_col, temps, sensors):
    tiers, snaps, width = temps.shape
    sens = sensors.shape[1]
    depth = tiers * snaps
    n_chunk = sens // (SUB * n_row)
    rows_out = sens // n_col
    rows_col = rows_out // n_chunk
    bf16 = jnp.bfloat16
    return pl.pallas_call(
        functools.partial(kernel, n_row, n_col, n_chunk, tiers),
        out_shape=jax.ShapeDtypeStruct((rows_out, n_col * width), bf16),
        in_specs=[pl.BlockSpec(memory_space=pltpu.VMEM)] * 2,
        out_specs=pl.BlockSpec(memory_space=pltpu.VMEM),
        scratch_shapes=[
            pltpu.VMEM((n_col, n_chunk, rows_col, tiers), jnp.int32),
            pltpu.VMEM((n_chunk, n_row, SUB, depth), bf16),
            pltpu.VMEM((n_chunk, n_row - 1, SUB, depth), bf16),
            pltpu.VMEM((n_chunk, SUB, depth), bf16),
            pltpu.VMEM((n_chunk, n_col - 1, SUB, depth), bf16),
            pltpu.VMEM((n_chunk, n_row, SUB, depth), bf16),
            pltpu.VMEM((n_chunk, n_col, rows_col, width), bf16),
        ] + [pltpu.SemaphoreType.DMA((n_chunk,))] * 8,
        compiler_params=pltpu.CompilerParams(collective_id=0, has_side_effects=True),
    )(temps.reshape(depth, width), sensors)


def solution(mesh):
    placed = (P(None, None, ("row", "col")), P())
    return jax.shard_map(
        functools.partial(body, mesh.shape["row"], mesh.shape["col"]),
        mesh=mesh, in_specs=placed, out_specs=P("col", "row"), check_vma=False,
    )
```

```python
import functools

import jax
import numpy as np
import jax.numpy as jnp
from jax import lax
from jax.experimental import pallas as pl
from jax.experimental.pallas import tpu as pltpu
from jax.sharding import PartitionSpec as P

SUB = 16
MESH = pl.DeviceIdType.MESH


def kernel(
    n_row, n_col, n_chunk, tiers,
    temps_hbm, sens_ref, out_ref,
    temps_ref, sens_t, part, core_buf, pair_sum, rs_buf, z_src, z_buf, full, out_buf,
    c_send, c_recv, rs_send, rs_recv, z_send, z_recv,
    ag_send, ag_recv, d_send, d_recv, o_send, o_recv, t_sem,
):
    r = lax.axis_index("row")
    z = lax.axis_index("col")
    core, chip = lax.rem(r, 2), r // 2
    other = 1 - core
    n_chip = n_row // 2
    snaps, width = temps_ref.shape[0] // tiers, temps_ref.shape[1]
    depth = temps_ref.shape[0]
    rows_col = out_ref.shape[0] // n_chunk
    half = rows_col // 2
    rows_half = n_chip * SUB
    scale = float(np.float32(1.0) / np.sqrt(np.float32(depth)))
    partner = (chip * 2 + other, z)

    def chip_peer(d):
        peer = lax.rem(chip + d, n_chip)
        return peer, (peer * 2 + core, z)

    n_half = n_col // 2
    side = z // n_half

    def col_peer(e):
        return lax.rem(z + e, n_col)

    def out_peer(e):
        across = (1 - side) * n_half + lax.rem(z + e, n_half)
        beside = side * n_half + lax.rem(z + e, n_half)
        return across if e < n_half else beside

    load = pltpu.make_async_copy(temps_hbm, temps_ref, t_sem)
    load.start()
    barrier = pltpu.get_barrier_semaphore()
    pl.semaphore_signal(barrier, inc=1, device_id=partner, device_id_type=MESH)
    for d in range(1, n_chip):
        pl.semaphore_signal(barrier, inc=1, device_id=chip_peer(d)[1], device_id_type=MESH)
    for e in range(1, n_col):
        pl.semaphore_signal(barrier, inc=1, device_id=(r, col_peer(e)), device_id_type=MESH)

    first_pixel = (r * n_col + z) * width
    offsets = jnp.transpose(sens_ref[...] - first_pixel)
    sens_t[...] = offsets.reshape(sens_t.shape)
    pixel_ids = lax.broadcasted_iota(jnp.int32, (rows_half, width), 1)

    def wait_all(ref, sem):
        pltpu.make_async_copy(ref, ref, sem).wait()

    def select(k):
        for h in range(2):
            mine = sens_t[:, k, h].reshape(rows_half, tiers)
            for t in range(0, tiers, 2):
                pair = []
                for u in (t, t + 1):
                    hot = (pixel_ids == mine[:, u:u + 1]).astype(jnp.float32).astype(jnp.bfloat16)
                    pair.append(lax.dot_general(
                        hot, temps_ref[u * snaps:(u + 1) * snaps, :],
                        (((1,), (1,)), ((), ())), preferred_element_type=jnp.float32,
                    ))
                both = jnp.concatenate(pair, axis=1).astype(jnp.bfloat16)
                part[k, h, :, :, t * snaps:(t + 2) * snaps] = both.reshape(n_chip, SUB, 2 * snaps)

    def start_core(k):
        pltpu.make_async_remote_copy(
            part.at[k, other], core_buf.at[k], c_send.at[k], c_recv.at[k],
            device_id=partner, device_id_type=MESH,
        ).start()

    def start_rs(k):
        wait_all(core_buf.at[k], c_recv.at[k])
        pair_sum[k] = part[k, core] + core_buf[k]
        for d in range(1, n_chip):
            peer, device = chip_peer(d)
            pltpu.make_async_remote_copy(
                pair_sum.at[k, peer], rs_buf.at[k, d - 1], rs_send.at[k], rs_recv.at[k],
                device_id=device, device_id_type=MESH,
            ).start()

    def start_z(k):
        wait_all(rs_buf.at[k], rs_recv.at[k])
        total = pair_sum[k, chip]
        for d in range(n_chip - 1):
            total = total + rs_buf[k, d]
        z_src[k] = total
        for e in range(1, n_col):
            pltpu.make_async_remote_copy(
                z_src.at[k], z_buf.at[k, e - 1], z_send.at[k], z_recv.at[k],
                device_id=(r, col_peer(e)), device_id_type=MESH,
            ).start()

    def start_ag(k):
        wait_all(z_buf.at[k], z_recv.at[k])
        total = z_src[k]
        for e in range(n_col - 1):
            total = total + z_buf[k, e]
        full[k, core, chip] = total
        for d in range(1, n_chip):
            pltpu.make_async_remote_copy(
                full.at[k, core, chip], full.at[k, core, chip], ag_send.at[k], ag_recv.at[k],
                device_id=chip_peer(d)[1], device_id_type=MESH,
            ).start()

    def start_pass(k):
        wait_all(rs_buf.at[k], ag_recv.at[k])
        pltpu.make_async_remote_copy(
            full.at[k, core], full.at[k, core], d_send.at[k], d_recv.at[k],
            device_id=partner, device_id_type=MESH,
        ).start()

    def start_out(k):
        wait_all(core_buf.at[k], d_recv.at[k])
        readings = full[k].reshape(2 * rows_half, depth)
        summed = jnp.dot(readings, temps_ref[...], preferred_element_type=jnp.float32)
        rounded = (summed * scale).astype(jnp.bfloat16)
        for h in range(2):
            out_buf[k, :, h * half:(h + 1) * half] = rounded[h * rows_half:(h + 1) * rows_half].reshape(n_col, half, width)
        rows = pl.ds(k * rows_col, rows_col)
        columns = pl.ds(pl.multiple_of(z * width, width), width)
        for e in [*range(n_half), *range(n_half + 1, n_col)]:
            peer = out_peer(e)
            pltpu.make_async_remote_copy(
                out_buf.at[k, peer], out_ref.at[rows, columns], o_send.at[k], o_recv.at[k],
                device_id=(r, peer), device_id_type=MESH,
            ).start()
        out_ref[rows, columns] = out_buf[k, z]

    load.wait()
    select(0)
    pl.semaphore_wait(barrier, n_chip + n_col - 1)
    start_core(0)
    for k in range(1, n_chunk):
        select(k)
        start_core(k)
        start_rs(k - 1)
    start_rs(n_chunk - 1)
    stages = (start_z, start_ag, start_pass, start_out)
    due = [(at + 3.0 * k, late, k) for late, at in enumerate((0, 4.5, 8, 9.2)) for k in range(n_chunk)]
    for _, late, k in sorted(due):
        stages[late](k)
    for k in range(n_chunk):
        wait_all(out_buf.at[k, pl.ds(0, n_col - 1)], o_recv.at[k])
        wait_all(core_buf.at[k], c_send.at[k])
        wait_all(rs_buf.at[k], rs_send.at[k])
        wait_all(z_buf.at[k], z_send.at[k])
        wait_all(rs_buf.at[k], ag_send.at[k])
        wait_all(core_buf.at[k], d_send.at[k])
        wait_all(out_buf.at[k, pl.ds(0, n_col - 1)], o_send.at[k])


def body(n_row, n_col, temps, sensors):
    tiers, snaps, width = temps.shape
    sens = sensors.shape[1]
    depth = tiers * snaps
    n_chunk = sens // (SUB * n_row)
    n_chip = n_row // 2
    rows_out = sens // n_col
    rows_col = rows_out // n_chunk
    bf16 = jnp.bfloat16
    return pl.pallas_call(
        functools.partial(kernel, n_row, n_col, n_chunk, tiers),
        out_shape=pltpu.VMEM((rows_out, n_col * width), bf16),
        in_specs=[pl.BlockSpec(memory_space=pl.ANY), pl.BlockSpec(memory_space=pltpu.VMEM)],
        out_specs=pl.BlockSpec(memory_space=pltpu.VMEM),
        scratch_shapes=[
            pltpu.VMEM((depth, width), bf16),
            pltpu.VMEM((n_col, n_chunk, 2, rows_col // 2, tiers), jnp.int32),
            pltpu.VMEM((n_chunk, 2, n_chip, SUB, depth), bf16),
            pltpu.VMEM((n_chunk, n_chip, SUB, depth), bf16),
            pltpu.VMEM((n_chunk, n_chip, SUB, depth), bf16),
            pltpu.VMEM((n_chunk, n_chip - 1, SUB, depth), bf16),
            pltpu.VMEM((n_chunk, SUB, depth), bf16),
            pltpu.VMEM((n_chunk, n_col - 1, SUB, depth), bf16),
            pltpu.VMEM((n_chunk, 2, n_chip, SUB, depth), bf16),
            pltpu.VMEM((n_chunk, n_col, rows_col, width), bf16),
        ] + [pltpu.SemaphoreType.DMA((n_chunk,))] * 12 + [pltpu.SemaphoreType.DMA],
        compiler_params=pltpu.CompilerParams(collective_id=0, has_side_effects=True),
    )(temps.reshape(depth, width), sensors)


def solution(mesh):
    placed = (P(None, None, ("row", "col")), P())
    return jax.shard_map(
        functools.partial(body, mesh.shape["row"], mesh.shape["col"]),
        mesh=mesh, in_specs=placed, out_specs=P("col", "row"), check_vma=False,
    )
```
